32 devices in a mesh: dp: 2 (over x), tp2: 4 (over z), tp: 4 (over y, core).
Axes of the slice: x: 2, y: 2, z: 4, core: 2. Of those that a mesh axis runs over, the one named last changes fastest.
Arguments:
- hidden: bfloat16 [2048, 4096], P('dp'), parts along dimension 0
- w_gate: bfloat16 [4096, 14336], P(None, ('tp2', 'tp'))
- w_up: bfloat16 [4096, 14336], P(None, ('tp2', 'tp'))
- w_down: bfloat16 [14336, 4096], P(('tp2', 'tp'))
- norm_gain: float32 [4096], replicated
- w_vocab: bfloat16 [4096, 32768], P(None, ('tp2', 'tp'))
- temperature: float32 [2048], P('dp'), parts along dimension 0
- target_ids: int32 [2048], P('dp'), parts along dimension 0
Outputs:
- output 1: float32 [2048], P('dp'), parts along dimension 0
- output 2: float32 [2048], P('dp'), parts along dimension 0
- output 3: float32 [2048], P('dp'), parts along dimension 0
- output 4: bfloat16 [2048, 32768], P('dp', ('tp2', 'tp')), parts along dimension 0
There are 2 independent parts. The reference program is written for one: setup_inputs(seed, part) draws one part's arguments, and reference() takes and returns one part's arrays. A program takes and returns all parts, laid end to end along the dimension named above; an argument that names none is the same for every part.
All inputs are finite; a program needn't handle non-finite values.
Results may differ from the reference program's by a relative error of at most 0.00397131.
Values are sent between devices in bfloat16 or wider.
A program may use at most 1 GiB of HBM per device.

```python
import jax
import jax.numpy as jnp
from jax import lax

BATCH_ROWS = 1024
D_MODEL = 4096
D_FF = 14336
VOCAB_SIZE = 32768
ROW_BLOCK = 8
NORM_EPS = 1e-6


def setup_inputs(seed: int = 0, part: int = 0) -> dict:
    base_key = jax.random.key(seed)
    part_key = jax.random.fold_in(base_key, part)
    shared = jax.random.split(base_key, 6)
    own_keys = jax.random.split(part_key, 3)
    hidden = jax.random.normal(own_keys[0], (BATCH_ROWS, D_MODEL), jnp.float32)
    w_gate = jax.random.normal(shared[0], (D_MODEL, D_FF), jnp.float32) * D_MODEL ** -0.5
    w_up = jax.random.normal(shared[1], (D_MODEL, D_FF), jnp.float32) * D_MODEL ** -0.5
    w_down = jax.random.normal(shared[2], (D_FF, D_MODEL), jnp.float32) * (2.0 * D_FF ** -0.5)
    norm_gain = jax.random.uniform(shared[3], (D_MODEL,), jnp.float32, 0.5, 1.5)
    col_scale = jnp.exp(0.3 * jax.random.normal(shared[4], (1, VOCAB_SIZE), jnp.float32))
    w_vocab = jax.random.normal(shared[5], (D_MODEL, VOCAB_SIZE), jnp.float32) * D_MODEL ** -0.5 * col_scale
    temperature = jax.random.uniform(own_keys[1], (BATCH_ROWS,), jnp.float32, 0.5, 2.0)
    target_ids = jax.random.randint(own_keys[2], (BATCH_ROWS,), 0, VOCAB_SIZE, jnp.int32)
    return {
        'hidden': hidden.astype(jnp.bfloat16),
        'w_gate': w_gate.astype(jnp.bfloat16),
        'w_up': w_up.astype(jnp.bfloat16),
        'w_down': w_down.astype(jnp.bfloat16),
        'norm_gain': norm_gain,
        'w_vocab': w_vocab.astype(jnp.bfloat16),
        'temperature': temperature,
        'target_ids': target_ids,
    }


def reference(hidden, w_gate, w_up, w_down, norm_gain, w_vocab, temperature, target_ids):
    gate_pre = jnp.dot(hidden, w_gate, preferred_element_type=jnp.float32)
    up_pre = jnp.dot(hidden, w_up, preferred_element_type=jnp.float32)
    hidden_act = (jax.nn.silu(gate_pre) * up_pre).astype(jnp.bfloat16)
    mlp_out = jnp.dot(hidden_act, w_down, preferred_element_type=jnp.float32).astype(jnp.bfloat16)
    resid_sum = hidden.astype(jnp.float32) + mlp_out.astype(jnp.float32)
    inv_rms = lax.rsqrt(jnp.mean(resid_sum * resid_sum, axis=-1, keepdims=True) + NORM_EPS)
    normed = (norm_gain * resid_sum * inv_rms).astype(jnp.bfloat16)
    num_blocks = BATCH_ROWS // ROW_BLOCK

    def head_block(block_in):
        block_x, block_temp, block_ids = block_in
        logits = jnp.dot(block_x, w_vocab, preferred_element_type=jnp.float32) / block_temp[:, None]
        row_max = jnp.max(logits, axis=-1, keepdims=True)
        shifted = jnp.exp(logits - row_max)
        sum_exp = jnp.sum(shifted, axis=-1)
        log_norm = row_max[:, 0] + jnp.log(sum_exp)
        mean_logit = jnp.sum(shifted * logits, axis=-1) / sum_exp
        target_logit = jnp.take_along_axis(logits, block_ids[:, None], axis=-1)[:, 0]
        logprobs = (logits - log_norm[:, None]).astype(jnp.bfloat16)
        return log_norm, log_norm - mean_logit, target_logit - log_norm, logprobs

    log_norm, entropy, target_logp, logprobs = lax.map(
        head_block,
        (normed.reshape(num_blocks, ROW_BLOCK, D_MODEL),
         temperature.reshape(num_blocks, ROW_BLOCK),
         target_ids.reshape(num_blocks, ROW_BLOCK)))
    return (log_norm.reshape(BATCH_ROWS), entropy.reshape(BATCH_ROWS),
            target_logp.reshape(BATCH_ROWS), logprobs.reshape(BATCH_ROWS, VOCAB_SIZE))
```

```python
import functools

import jax
import jax.numpy as jnp
from jax import lax
from jax.experimental import pallas as pl
from jax.experimental.pallas import tpu as pltpu
from jax.sharding import PartitionSpec as P

NORM_EPS = 1e-6
MESH = pl.DeviceIdType.MESH
F32 = jnp.float32
BF16 = jnp.bfloat16

CHUNK = 256
HALF = 128
PIECE = 16
UNITS = 6
GROUP = 16
OFF_A = (0, 2, 4, 6, 8, 10, 12, 13)
OFF_B = (0, 0, 2, 4, 6, 8, 10, 11)
VOCAB_AT = 23
FINAL_AT = 28


def kernel(num_chunks, hidden, w_gate, w_up, w_down, gain, w_vocab, temp, ids,
           logprobs, log_norm, entropy, target_logp,
           w1, w2, wv, hid, act, dsend, drecv, acc, zbuf, cbuf, ybuf, xbuf, hres, logits, stat, sbuf, outb,
           w_sem, w2_sem, wv_sem, hid_sem, hres_sem, out_sem, d_send, d_recv,
           y_send, y_recv, z_send, z_recv, c_recv, x_send, x_recv, xy_recv, xd_send, xd_recv, s_send, s_recv):
    dim = hidden.shape[1]
    ff = w_gate.shape[1]
    vocab = w_vocab.shape[1]
    vt = vocab // 4
    dt = dim // 8
    num_units = num_chunks * UNITS
    ft = ff // 128

    dp = lax.axis_index('dp')
    z = lax.axis_index('tp2')
    t = lax.axis_index('tp')
    y = t // 2
    c = t % 2
    me = z * 4 + t
    is_leaf = (z % 3) == 0
    is_center = (z % 3) != 0
    adj = 1 + z // 3
    leaf = 3 * (z // 2)
    other = 3 - z
    core_dev = (dp, z, y * 2 + 1 - c)
    y_dev = (dp, z, (1 - y) * 2 + c)
    adj_dev = (dp, adj, t)
    leaf_dev = (dp, leaf, t)
    other_dev = (dp, other, t)

    def w1_copies(n):
        col = pl.multiple_of(n * 128, 128)
        at = pl.multiple_of(n * 256, 256)
        return (pltpu.make_async_copy(w_gate.at[:, pl.ds(col, 128)], w1.at[:, pl.ds(at, 128)], w_sem.at[n, 0]),
                pltpu.make_async_copy(w_up.at[:, pl.ds(col, 128)], w1.at[:, pl.ds(at + 128, 128)], w_sem.at[n, 1]))

    def w2_copy():
        return pltpu.make_async_copy(w_down, w2, w2_sem)

    def wv_copy(n):
        q = n % 4
        b = n % 2
        return pltpu.make_async_copy(w_vocab.at[:, pl.ds(pl.multiple_of(q * vt, vt), vt)], wv.at[b], wv_sem.at[b])

    def hid_copies(i):
        own = pl.multiple_of(i * CHUNK + c * HALF, HALF)
        oth = pl.multiple_of(i * CHUNK + (1 - c) * HALF, HALF)
        return (pltpu.make_async_copy(hidden.at[pl.ds(own, HALF)], hid.at[pl.ds(0, HALF)], hid_sem.at[0]),
                pltpu.make_async_copy(hidden.at[pl.ds(oth, HALF)], hid.at[pl.ds(HALF, HALF)], hid_sem.at[1]))

    def out_copies(i):
        own = pl.multiple_of(i * CHUNK + c * HALF, HALF)
        oth = pl.multiple_of(i * CHUNK + (1 - c) * HALF, HALF)
        return (pltpu.make_async_copy(outb.at[pl.ds(0, HALF)], logprobs.at[pl.ds(own, HALF)], out_sem.at[0]),
                pltpu.make_async_copy(outb.at[pl.ds(HALF, HALF)], logprobs.at[pl.ds(oth, HALF)], out_sem.at[1]))

    def remote(src, dst, send, recv, dev):
        return pltpu.make_async_remote_copy(src_ref=src, dst_ref=dst, send_sem=send, recv_sem=recv,
                                            device_id=dev, device_id_type=MESH)

    def d_copy(i, part):
        cols = pl.ds(part * (dim // 2), dim // 2)
        return remote(dsend.at[:, cols], drecv.at[i, :, cols], d_send.at[part], d_recv.at[i, part], core_dev)

    def geo(u, kind):
        i = u // UNITS
        k = u % UNITS
        m = k % 3
        rs = 64 * (k // 3) + 16 * m + 16 * ((m + 1) // 2)
        if kind == 'A':
            return i, k, rs, rs + PIECE * y, 1 + k // 3
        return i, k, rs, rs, m

    def rows(start, n=PIECE):
        return pl.ds(pl.multiple_of(start, PIECE), n)

    def y_index(i, k, kind):
        return i * 4 + k // 3 + (0 if kind == 'A' else 2)

    def c_index(i, k, kind):
        return i * 3 + (0 if kind == 'A' else 1 + k // 3)

    def ya_copy(u):
        i, k, rs, mr, zo = geo(u, 'A')
        n = y_index(i, k, 'A')
        return remote(acc.at[i, rows(rs + PIECE * (1 - y))], ybuf.at[n], y_send.at[u], y_recv.at[n], y_dev)

    def yb_copy(u):
        i, k, rs, mr, zo = geo(u, 'B')
        n = y_index(i, k, 'B')
        return remote(acc.at[i, rows(mr)], ybuf.at[n], y_send.at[u], y_recv.at[n], y_dev)

    def z_copy(u, kind):
        i, k, rs, mr, zo = geo(u, kind)
        return remote(acc.at[i, rows(mr)], zbuf.at[u], z_send.at[u], z_recv.at[u], adj_dev)

    def c_copy(u, kind):
        i, k, rs, mr, zo = geo(u, kind)
        n = c_index(i, k, kind)
        return remote(acc.at[i, rows(mr)], cbuf.at[n], z_send.at[u], c_recv.at[n], other_dev)

    def x_copy(u, kind, which):
        i, k, rs, mr, zo = geo(u, kind)
        block = xbuf.at[i, rows(mr)]
        dev = (leaf_dev, other_dev, y_dev)[which]
        recv = xy_recv.at[u // 3] if which == 2 else x_recv.at[u]
        return remote(block, block, x_send.at[u, which], recv, dev)

    def xy_wait(u):
        i, k, rs, mr, zo = geo(u, 'A')
        block = xbuf.at[i, rows(rs + PIECE * (1 - y))]
        return remote(block, block, x_send.at[u, 2], xy_recv.at[u // 3], y_dev)

    def xd_copy(u, kind):
        i, k, rs, mr, zo = geo(u, kind)
        n = 2 * PIECE if kind == 'A' else PIECE
        return remote(xbuf.at[i, rows(rs, n)], xbuf.at[i, rows(HALF + rs, n)], xd_send.at[u], xd_recv.at[u], core_dev)

    def hres_copy(u, kind):
        i, k, rs, mr, zo = geo(u, kind)
        row = pl.multiple_of(i * CHUNK + c * HALF + mr, PIECE)
        return pltpu.make_async_copy(hidden.at[pl.ds(row, PIECE)], hres.at[u % 8], hres_sem.at[u % 8])

    cb = min(dim, 1024)

    def add_rows(i, start, n, *terms):
        for j in range(dim // cb):
            cols = pl.ds(j * cb, cb)
            total = acc[i, rows(start, n), cols].astype(F32)
            for ref in terms:
                total = total + ref[:, cols].astype(F32)
            acc[i, rows(start, n), cols] = total.astype(BF16)

    def norm_rows(u, kind, *terms):
        i, k, rs, mr, zo = geo(u, kind)
        slot = hres.at[u % 8]
        hres_copy(u, kind).wait()
        square = jnp.zeros((PIECE, 128), F32)
        for j in range(dim // cb):
            cols = pl.ds(j * cb, cb)
            total = acc[i, rows(mr), cols].astype(F32)
            for ref in terms:
                total = total + ref[:, cols].astype(F32)
            resid = slot[:, cols].astype(F32) + total.astype(BF16).astype(F32)
            sq = resid * resid
            for b in range(cb // 128):
                square = square + sq[:, b * 128:(b + 1) * 128]
            xbuf[i, rows(mr), cols] = total.astype(BF16)
        inv = lax.rsqrt(jnp.sum(square, axis=-1, keepdims=True) / dim + NORM_EPS)
        for j in range(dim // cb):
            cols = pl.ds(j * cb, cb)
            resid = slot[:, cols].astype(F32) + xbuf[i, rows(mr), cols].astype(F32)
            xbuf[i, rows(mr), cols] = (gain[:, cols] * resid * inv).astype(BF16)

    def s_copy(i, d):
        peer = (me + d) % GROUP
        return remote(sbuf.at[i, 0], sbuf.at[i, d], s_send.at[i], s_recv.at[i], (dp, peer // 4, peer % 4))

    def s_wait(i):
        block = sbuf.at[i, pl.ds(1, GROUP - 1)]
        return remote(block, block, s_send.at[i], s_recv.at[i], core_dev)

    for cp in hid_copies(0):
        cp.start()

    def load_w1(n, _):
        for cp in w1_copies(n):
            cp.start()
        return 0
    lax.fori_loop(0, ft, load_w1, 0)
    w2_copy().start()
    wv_copy(0).start()
    wv_copy(1).start()

    barrier = pltpu.get_barrier_semaphore()

    def greet(d, _):
        peer = (me + d) % GROUP
        pl.semaphore_signal(barrier, inc=1, device_id=(dp, peer // 4, peer % 4), device_id_type=MESH)
        return 0
    lax.fori_loop(1, GROUP, greet, 0)
    pl.semaphore_wait(barrier, GROUP - 1)

    def gate_up(i, j):
        def tile(n, _):
            @pl.when(i == 0)
            def _():
                for cp in w1_copies(n):
                    cp.wait()
            at = pl.multiple_of(n * 256, 256)
            both = jnp.dot(hid[...], w1[:, pl.ds(at, 256)], preferred_element_type=F32)
            g = both[:, :128]
            act[:, pl.ds(pl.multiple_of(n * 128, 128), 128)] = (jax.nn.silu(g) * both[:, 128:]).astype(BF16)
            return 0
        per = -(-ft // 4)
        lax.fori_loop(j * per, jnp.minimum(j * per + per, ft), tile, 0)

    def down(i, part):
        def tile(n, _):
            cols = pl.ds(pl.multiple_of(n * dt, dt), dt)
            out = jnp.dot(act[...], w2[:, cols], preferred_element_type=F32).astype(BF16)
            acc[i, :, cols] = out[:HALF]
            dsend[:, cols] = out[HALF:]
            return 0
        lax.fori_loop(part * 4, part * 4 + 4, tile, 0)

    def mlp(s):
        i = s // UNITS
        j = s % UNITS

        @pl.when(j == 0)
        def _():
            for cp in hid_copies(i):
                cp.wait()

        @pl.when(j < 4)
        def _():
            gate_up(i, j)

        @pl.when((j == 3) & (i + 1 < num_chunks))
        def _():
            for cp in hid_copies(i + 1):
                cp.start()

        @pl.when((j == 4) & (i == 0))
        def _():
            w2_copy().wait()

        @pl.when((j == 4) & (i > 0))
        def _():
            d_copy(i - 1, 0).wait_send()
            d_copy(i - 1, 1).wait_send()

        @pl.when(j >= 4)
        def _():
            down(i, j - 4)

        @pl.when(j == 4)
        def _():
            d_copy(i, 0).start()

        @pl.when(j == 5)
        def _():
            d_copy(i, 1).start()

    def column(row_ref, i, h):
        r = row_ref[pl.ds(2 * i + (c if h == 0 else 1 - c), 1), :].astype(F32)
        return jnp.transpose(jnp.broadcast_to(r, (128, 128)))

    lanes = 128
    rb = 32

    def vocab_step(i, q):
        n = i * 4 + q
        wv_copy(n).wait()
        col = pl.multiple_of(q * vt, vt)
        logits[:, pl.ds(col, vt)] = jnp.dot(xbuf[i], wv[n % 2], preferred_element_type=F32)

        @pl.when(n + 2 < num_chunks * 4)
        def _():
            wv_copy(n + 2).start()

        @pl.when(q == 0)
        def _():
            for h in range(2):
                r = pl.ds(h * HALF, HALF)
                stat[0, r] = jnp.full((HALF, lanes), -jnp.inf, F32)
                stat[1, r] = jnp.zeros((HALF, lanes), F32)
                stat[2, r] = jnp.zeros((HALF, lanes), F32)
                stat[3, r] = jnp.zeros((HALF, lanes), F32)
                stat[4, r] = 1.0 / column(temp, i, h)
                stat[5, r] = column(ids, i, h) - (me * vocab).astype(F32)

        def block(b, _):
            r = pl.ds(pl.multiple_of(b * rb, rb), rb)
            inv_t = stat[4, r]
            want = stat[5, r] - lax.broadcasted_iota(jnp.int32, (rb, lanes), 1).astype(F32) - (q * vt).astype(F32)
            old = stat[0, r]
            top = old
            parts = []
            target = stat[3, r]
            for g in range(vt // lanes):
                cols = pl.ds(pl.multiple_of(col + g * lanes, lanes), lanes)
                lg = logits[r, cols] * inv_t
                logits[r, cols] = lg
                top = jnp.maximum(top, lg)
                target = target + jnp.where(want == float(g * lanes), lg, 0.0)
                parts.append(lg)
            scale = jnp.exp(old - top)
            total = stat[1, r] * scale
            moment = stat[2, r] * scale
            for lg in parts:
                e = jnp.exp(lg - top)
                total = total + e
                moment = moment + e * lg
            stat[0, r] = top
            stat[1, r] = total
            stat[2, r] = moment
            stat[3, r] = target
            return 0
        lax.fori_loop(0, CHUNK // rb, block, 0)

        @pl.when(q == 3)
        def _():
            for h in range(2):
                r = pl.ds(h * HALF, HALF)
                top = stat[0, r]
                best = jnp.max(top, axis=-1, keepdims=True)
                w = jnp.exp(top - best)
                total = jnp.sum(stat[1, r] * w, axis=-1, keepdims=True)
                moment = jnp.sum(stat[2, r] * w, axis=-1, keepdims=True)
                target = jnp.sum(stat[3, r], axis=-1, keepdims=True)
                lane = lax.broadcasted_iota(jnp.int32, (HALF, lanes), 1)
                packed = jnp.where(lane == 0, best, jnp.where(lane == 1, total, jnp.where(lane == 2, moment, target)))
                turned = jnp.transpose(packed)[:8]
                at = pl.multiple_of((c if h == 0 else 1 - c) * HALF, HALF)
                sbuf[i, 0, :, pl.ds(at, HALF)] = turned
            for d in range(1, GROUP):
                s_copy(i, d).start()

    def final_step(i):
        s_wait(i).wait_recv()
        top = sbuf[i, 0, 0:1, :]
        for d in range(1, GROUP):
            top = jnp.maximum(top, sbuf[i, d, 0:1, :])
        total = jnp.zeros((1, CHUNK), F32)
        moment = jnp.zeros((1, CHUNK), F32)
        target = jnp.zeros((1, CHUNK), F32)
        for d in range(GROUP):
            w = jnp.exp(sbuf[i, d, 0:1, :] - top)
            total = total + w * sbuf[i, d, 1:2, :]
            moment = moment + w * sbuf[i, d, 2:3, :]
            target = target + sbuf[i, d, 3:4, :]
        norm = top + jnp.log(total)
        ent = norm - moment / total
        tlp = target - norm
        for h in range(2):
            r = pl.ds(2 * i + h, 1)
            cols = slice(h * HALF, (h + 1) * HALF)
            log_norm[r, :] = norm[:, cols]
            entropy[r, :] = ent[:, cols]
            target_logp[r, :] = tlp[:, cols]

        @pl.when(i > 0)
        def _():
            for cp in out_copies(i - 1):
                cp.wait()
        for h in range(2):
            row = column(log_norm, i, h)
            stat[0, pl.ds(h * HALF, HALF)] = row

        def block(b, _):
            r = pl.ds(pl.multiple_of(b * rb, rb), rb)
            ln = stat[0, r]
            for g in range(vocab // lanes):
                cols = pl.ds(g * lanes, lanes)
                outb[r, cols] = (logits[r, cols] - ln).astype(BF16)
            return 0
        lax.fori_loop(0, CHUNK // rb, block, 0)
        for cp in out_copies(i):
            cp.start()

    def unit(s, h, kind, body):
        off = (OFF_A if kind == 'A' else OFF_B)[h]
        u = s - UNITS - off
        fit = (u % 3) == 0 if kind == 'A' else (u % 3) != 0

        @pl.when((u >= 0) & (u < num_units) & fit)
        def _():
            body(u)

    def first(kind):
        def body(u):
            i, k, rs, mr, zo = geo(u, kind)
            if kind == 'A':
                @pl.when(k == 0)
                def _():
                    d_copy(i, 0).wait_recv()
                    d_copy(i, 1).wait_recv()
                add_rows(i, rs, 2 * PIECE, drecv.at[i, rows(rs, 2 * PIECE)])
                ya_copy(u).start()
            else:
                add_rows(i, rs, PIECE, drecv.at[i, rows(rs)])

                @pl.when(is_leaf)
                def _():
                    z_copy(u, kind).start()
        return body

    def after_y(u):
        i, k, rs, mr, zo = geo(u, 'A')
        ya_copy(u).wait_recv()
        add_rows(i, mr, PIECE, ybuf.at[y_index(i, k, 'A')])

        @pl.when(is_leaf)
        def _():
            z_copy(u, 'A').start()

    def after_z(kind):
        def body(u):
            i, k, rs, mr, zo = geo(u, kind)

            @pl.when(z == 3 - zo)
            def _():
                z_copy(u, kind).wait_recv()
                add_rows(i, mr, PIECE, zbuf.at[u])
                c_copy(u, kind).start()

            @pl.when(z == zo)
            def _():
                hres_copy(u, kind).start()
        return body

    def spread(u, kind):
        x_copy(u, kind, 0).start()
        x_copy(u, kind, 1).start()
        if kind == 'A':
            x_copy(u, kind, 2).start()

    def after_c(kind):
        def body(u):
            i, k, rs, mr, zo = geo(u, kind)

            @pl.when(z == zo)
            def _():
                z_copy(u, kind).wait_recv()
                c_copy(u, kind).wait_recv()
                n = c_index(i, k, kind)
                if kind == 'A':
                    norm_rows(u, kind, zbuf.at[u], cbuf.at[n])
                    spread(u, kind)
                else:
                    add_rows(i, mr, PIECE, zbuf.at[u], cbuf.at[n])
                    yb_copy(u).start()
        return body

    def after_yb(u):
        i, k, rs, mr, zo = geo(u, 'B')

        @pl.when(z == zo)
        def _():
            yb_copy(u).wait_recv()
            norm_rows(u, 'B', ybuf.at[y_index(i, k, 'B')])
            spread(u, 'B')

    def near(kind):
        def body(u):
            i, k, rs, mr, zo = geo(u, kind)

            @pl.when(z == 3 - zo)
            def _():
                x_copy(u, kind, 0).wait_recv()
                x_copy(u, kind, 0).start()
                if kind == 'A':
                    x_copy(u, kind, 2).start()

            @pl.when(z == 3 * (zo - 1))
            def _():
                x_copy(u, kind, 0).wait_recv()
                if kind == 'A':
                    x_copy(u, kind, 2).start()
        return body

    def far(kind):
        def body(u):
            i, k, rs, mr, zo = geo(u, kind)

            @pl.when(z == 3 * (2 - zo))
            def _():
                x_copy(u, kind, 0).wait_recv()
                if kind == 'A':
                    x_copy(u, kind, 2).start()
            if kind == 'B':
                xd_copy(u, kind).start()
        return body

    def after_xy(u):
        xy_wait(u).wait_recv()
        xd_copy(u, 'A').start()

    def after_xd(kind):
        def body(u):
            xd_copy(u, kind).wait_recv()
        return body

    def slot(s, _):
        unit(s, 7, 'A', after_xd('A'))
        unit(s, 7, 'B', after_xd('B'))
        unit(s, 6, 'A', after_xy)
        unit(s, 6, 'B', far('B'))
        unit(s, 5, 'A', far('A'))
        unit(s, 5, 'B', near('B'))
        unit(s, 4, 'A', near('A'))
        unit(s, 4, 'B', after_yb)
        unit(s, 3, 'A', after_c('A'))
        unit(s, 3, 'B', after_c('B'))
        unit(s, 2, 'A', after_z('A'))
        unit(s, 2, 'B', after_z('B'))
        unit(s, 1, 'A', after_y)
        unit(s, 0, 'A', first('A'))
        unit(s, 0, 'B', first('B'))

        f = s - FINAL_AT

        @pl.when((f >= 0) & (f % UNITS == 0))
        def _():
            final_step(f // UNITS)

        v = s - VOCAB_AT

        @pl.when((v >= 0) & (v % UNITS < 4) & (v < UNITS * num_chunks))
        def _():
            vocab_step(v // UNITS, v % UNITS)

        @pl.when(s < UNITS * num_chunks)
        def _():
            mlp(s)
        return 0

    last = UNITS * (num_chunks - 1) + FINAL_AT
    lax.fori_loop(0, last + 1, slot, 0)

    for cp in out_copies(num_chunks - 1):
        cp.wait()
    d_copy(num_chunks - 1, 0).wait_send()
    d_copy(num_chunks - 1, 1).wait_send()

    def drain_unit(u, kind):
        i, k, rs, mr, zo = geo(u, kind)
        xd_copy(u, kind).wait_send()
        if kind == 'A':
            ya_copy(u).wait_send()
            x_copy(u, kind, 2).wait_send()

        @pl.when(is_leaf)
        def _():
            z_copy(u, kind).wait_send()

        @pl.when(z == 3 - zo)
        def _():
            c_copy(u, kind).wait_send()
            x_copy(u, kind, 0).wait_send()

        @pl.when(z == zo)
        def _():
            if kind == 'B':
                yb_copy(u).wait_send()
            x_copy(u, kind, 0).wait_send()
            x_copy(u, kind, 1).wait_send()

    def drain(n, _):
        drain_unit(3 * n, 'A')
        drain_unit(3 * n + 1, 'B')
        drain_unit(3 * n + 2, 'B')
        return 0
    lax.fori_loop(0, num_units // 3, drain, 0)

    def drain_stats(i, _):
        s_wait(i).wait_send()
        return 0
    lax.fori_loop(0, num_chunks, drain_stats, 0)


def fused(hidden, w_gate, w_up, w_down, gain, w_vocab, temp, ids):
    rows, dim = hidden.shape
    ff = w_gate.shape[1]
    vocab = w_vocab.shape[1]
    nc = rows // CHUNK
    nu = nc * UNITS
    vm = pl.BlockSpec(memory_space=pltpu.VMEM)
    hbm = pl.BlockSpec(memory_space=pl.ANY)
    dma = pltpu.SemaphoreType.DMA
    small = jax.ShapeDtypeStruct((rows // 128, 128), F32)
    return pl.pallas_call(
        functools.partial(kernel, nc),
        out_shape=(jax.ShapeDtypeStruct((rows, vocab), BF16), small, small, small),
        in_specs=[hbm, hbm, hbm, hbm, vm, hbm, vm, vm],
        out_specs=(hbm, vm, vm, vm),
        scratch_shapes=[
            pltpu.VMEM((dim, 2 * ff), BF16),
            pltpu.VMEM((ff, dim), BF16),
            pltpu.VMEM((2, dim, vocab // 4), BF16),
            pltpu.VMEM((CHUNK, dim), BF16),
            pltpu.VMEM((CHUNK, ff), BF16),
            pltpu.VMEM((HALF, dim), BF16),
            pltpu.VMEM((nc, HALF, dim), BF16),
            pltpu.VMEM((nc, HALF, dim), BF16),
            pltpu.VMEM((nu, PIECE, dim), BF16),
            pltpu.VMEM((nc * 3, PIECE, dim), BF16),
            pltpu.VMEM((nc * 4, PIECE, dim), BF16),
            pltpu.VMEM((nc, CHUNK, dim), BF16),
            pltpu.VMEM((8, PIECE, dim), BF16),
            pltpu.VMEM((CHUNK, vocab), F32),
            pltpu.VMEM((6, CHUNK, 128), F32),
            pltpu.VMEM((nc, GROUP, 8, CHUNK), F32),
            pltpu.VMEM((CHUNK, vocab), BF16),
            dma((ff // 128, 2)), dma, dma((2,)), dma((2,)), dma((8,)), dma((2,)), dma((2,)), dma((nc, 2)),
            dma((nu,)), dma((nc * 4,)), dma((nu,)), dma((nu,)), dma((nc * 3,)), dma((nu, 3)), dma((nu,)),
            dma((nu // 3,)), dma((nu,)), dma((nu,)), dma((nc,)), dma((nc,)),
        ],
        compiler_params=pltpu.CompilerParams(collective_id=0, has_side_effects=True, vmem_limit_bytes=67043328),
        cost_estimate=pl.CostEstimate(flops=2 * rows * dim * (3 * ff + vocab),
                                      bytes_accessed=2 * dim * (3 * ff + 4 * vocab + rows),
                                      transcendentals=rows * vocab),
        name='step_tail',
    )(hidden, w_gate, w_up, w_down, gain, w_vocab, temp, ids)


def solution(mesh):
    model_axes = ('tp2', 'tp')

    def local_step(hidden, w_gate, w_up, w_down, norm_gain, w_vocab, temperature, target_ids):
        rows = hidden.shape[0]
        logprobs, log_norm, entropy, target_logp = fused(
            hidden, w_gate, w_up, w_down, norm_gain[None, :], w_vocab,
            temperature.reshape(rows // 128, 128), target_ids.reshape(rows // 128, 128))
        return log_norm.reshape(rows), entropy.reshape(rows), target_logp.reshape(rows), logprobs

    return jax.shard_map(
        local_step, mesh=mesh,
        in_specs=(P('dp', None), P(None, model_axes), P(None, model_axes), P(model_axes, None),
                  P(None), P(None, model_axes), P('dp'), P('dp')),
        out_specs=(P('dp'), P('dp'), P('dp'), P('dp', model_axes)),
        check_vma=False)
```

```python
import functools

import jax
import jax.numpy as jnp
from jax import lax
from jax.experimental import pallas as pl
from jax.experimental.pallas import tpu as pltpu
from jax.sharding import PartitionSpec as P

NORM_EPS = 1e-6
MESH = pl.DeviceIdType.MESH
F32 = jnp.float32
BF16 = jnp.bfloat16

CHUNK = 256
HALF = 128
PIECE = 16
UNITS = 6
GROUP = 16
KINDS = 'ABBABB'
POS_UNIT = (
    (6.295, 9.934, 14.066, 22.525, 29.115, 34.033, 39.443, 42.984, 46.131),
    (6.59, 9.639, 19.18, 22.721, 26.951, 35.213, 43.672, 44.754),
    (7.377, 10.23, 14.164, 17.508, 21.148, 25.77, 33.738, 45.049),
    (7.475, 11.607, 17.902, 23.705, 29.803, 36.885, 39.541, 42.492, 47.016),
    (8.262, 12.393, 18.098, 22.623, 27.246, 33.344, 37.869, 46.426),
    (8.852, 13.574, 19.279, 23.311, 30.689, 38.557, 42.787, 46.918),
)
POS_MLP = (0.197, 1.967, 2.361, 2.656, 4.328, 4.82)
POS_VOCAB = (48, 49.082, 50.459, 53.41)
POS_FINAL = 57.836

def kernel(num_chunks, hidden, w_gate, w_up, w_down, gain, w_vocab, temp, ids,
           logprobs, log_norm, entropy, target_logp,
           w1, w2, wv, hid, act, dsend, drecv, acc, zbuf, cbuf, ybuf, xbuf, hres, logits, stat, sbuf, outb,
           w_sem, w2_sem, wv_sem, hid_sem, hres_sem, out_sem, d_send, d_recv,
           y_send, y_recv, z_send, z_recv, c_recv, x_send, x_recv, xy_recv, xd_send, xd_recv, s_send, s_recv):
    dim = hidden.shape[1]
    ff = w_gate.shape[1]
    vocab = w_vocab.shape[1]
    vt = vocab // 4
    dt = dim // 8
    num_units = num_chunks * UNITS
    ft = ff // 128

    dp = lax.axis_index('dp')
    z = lax.axis_index('tp2')
    t = lax.axis_index('tp')
    y = t // 2
    c = t % 2
    me = z * 4 + t
    core_dev = (dp, z, y * 2 + 1 - c)
    y_dev = (dp, z, (1 - y) * 2 + c)
    def dist(zo):
        return z if zo < 2 else 3 - z

    def step_dev(zo, way):
        there = z - way if zo < 2 else z + way
        return (dp, jnp.clip(there, 0, 3), t)

    def w1_copies(n):
        col = pl.multiple_of(n * 128, 128)
        at = pl.multiple_of(n * 256, 256)
        return (pltpu.make_async_copy(w_gate.at[:, pl.ds(col, 128)], w1.at[:, pl.ds(at, 128)], w_sem.at[n, 0]),
                pltpu.make_async_copy(w_up.at[:, pl.ds(col, 128)], w1.at[:, pl.ds(at + 128, 128)], w_sem.at[n, 1]))

    def w2_copy():
        return pltpu.make_async_copy(w_down, w2, w2_sem)

    def wv_copy(n):
        q = n % 4
        b = n % 2
        return pltpu.make_async_copy(w_vocab.at[:, pl.ds(pl.multiple_of(q * vt, vt), vt)], wv.at[b], wv_sem.at[b])

    def hid_copies(i):
        own = pl.multiple_of(i * CHUNK + c * HALF, HALF)
        oth = pl.multiple_of(i * CHUNK + (1 - c) * HALF, HALF)
        return (pltpu.make_async_copy(hidden.at[pl.ds(own, HALF)], hid.at[pl.ds(0, HALF)], hid_sem.at[0]),
                pltpu.make_async_copy(hidden.at[pl.ds(oth, HALF)], hid.at[pl.ds(HALF, HALF)], hid_sem.at[1]))

    def out_copies(i):
        own = pl.multiple_of(i * CHUNK + c * HALF, HALF)
        oth = pl.multiple_of(i * CHUNK + (1 - c) * HALF, HALF)
        return (pltpu.make_async_copy(outb.at[pl.ds(0, HALF)], logprobs.at[pl.ds(own, HALF)], out_sem.at[0]),
                pltpu.make_async_copy(outb.at[pl.ds(HALF, HALF)], logprobs.at[pl.ds(oth, HALF)], out_sem.at[1]))

    def remote(src, dst, send, recv, dev):
        return pltpu.make_async_remote_copy(src_ref=src, dst_ref=dst, send_sem=send, recv_sem=recv,
                                            device_id=dev, device_id_type=MESH)

    def d_copy(i, part):
        start = part * (dim // 2)
        cols = pl.ds(start if isinstance(part, int) else pl.multiple_of(start, dim // 2), dim // 2)
        return remote(dsend.at[:, cols], drecv.at[i, :, cols], d_send.at[part], d_recv.at[i, part], core_dev)

    def geo(u, kind):
        i, k = u
        m = k % 3
        rs = 64 * (k // 3) + 16 * m + 16 * ((m + 1) // 2)
        if kind == 'A':
            return i, k, rs, rs + PIECE * y, 3 * (k // 3)
        return i, k, rs, rs, m if kind == 'C' else 3 * (m - 1)

    def flat(u):
        return u[0] * UNITS + u[1]

    def rows(start, n=PIECE):
        return pl.ds(pl.multiple_of(start, PIECE), n)

    def y_index(i, k, kind):
        return i * 4 + k // 3 + (0 if kind == 'A' else 2)

    def ya_copy(u):
        i, k, rs, mr, zo = geo(u, 'A')
        n = y_index(i, k, 'A')
        return remote(acc.at[i, rows(rs + PIECE * (1 - y))], ybuf.at[n], y_send.at[flat(u)], y_recv.at[n], y_dev)

    def yb_copy(u, kind):
        i, k, rs, mr, zo = geo(u, kind)
        n = y_index(i, k, 'B')
        return remote(acc.at[i, rows(mr)], ybuf.at[n], y_send.at[flat(u)], y_recv.at[n], y_dev)

    def z_copy(u, kind):
        i, k, rs, mr, zo = geo(u, kind)
        return remote(acc.at[i, rows(mr)], zbuf.at[flat(u)], z_send.at[flat(u)], z_recv.at[flat(u)], step_dev(zo, 1))

    def x_copy(u, kind):
        i, k, rs, mr, zo = geo(u, kind)
        block = xbuf.at[i, rows(mr)]
        return remote(block, block, x_send.at[flat(u), 0], x_recv.at[flat(u)], step_dev(zo, -1))

    def c_copy(u):
        i, k, rs, mr, zo = geo(u, 'C')
        return remote(acc.at[i, rows(mr)], cbuf.at[i], z_send.at[flat(u)], c_recv.at[i], step_dev(zo, -1))

    def xn_copy(u):
        i, k, rs, mr, zo = geo(u, 'C')
        block = xbuf.at[i, rows(mr)]
        return remote(block, block, x_send.at[flat(u), 1], x_recv.at[flat(u)], step_dev(zo, 1))

    def xy_copy(u):
        i, k, rs, mr, zo = geo(u, 'A')
        block = xbuf.at[i, rows(mr)]
        return remote(block, block, x_send.at[flat(u), 1], xy_recv.at[flat(u) // 3], y_dev)

    def xy_wait(u):
        i, k, rs, mr, zo = geo(u, 'A')
        block = xbuf.at[i, rows(rs + PIECE * (1 - y))]
        return remote(block, block, x_send.at[flat(u), 1], xy_recv.at[flat(u) // 3], y_dev)

    def xd_copy(u, kind):
        i, k, rs, mr, zo = geo(u, kind)
        n = 2 * PIECE if kind == 'A' else PIECE
        return remote(xbuf.at[i, rows(rs, n)], xbuf.at[i, rows(HALF + rs, n)], xd_send.at[flat(u)], xd_recv.at[flat(u)], core_dev)

    def hres_copy(u, kind):
        i, k, rs, mr, zo = geo(u, kind)
        row = pl.multiple_of(i * CHUNK + c * HALF + mr, PIECE)
        return pltpu.make_async_copy(hidden.at[pl.ds(row, PIECE)], hres.at[flat(u) % 12], hres_sem.at[flat(u) % 12])

    cb = min(dim, 1024)

    def add_rows(i, start, n, *terms):
        for j in range(dim // cb):
            cols = pl.ds(j * cb, cb)
            total = acc[i, rows(start, n), cols].astype(F32)
            for ref in terms:
                total = total + ref[:, cols].astype(F32)
            acc[i, rows(start, n), cols] = total.astype(BF16)

    def norm_rows(u, kind, *terms):
        i, k, rs, mr, zo = geo(u, kind)
        slot = hres.at[flat(u) % 12]
        hres_copy(u, kind).wait()
        square = jnp.zeros((PIECE, 128), F32)
        for j in range(dim // cb):
            cols = pl.ds(j * cb, cb)
            total = acc[i, rows(mr), cols].astype(F32)
            for ref in terms:
                total = total + ref[:, cols].astype(F32)
            resid = slot[:, cols].astype(F32) + total.astype(BF16).astype(F32)
            sq = resid * resid
            for b in range(cb // 128):
                square = square + sq[:, b * 128:(b + 1) * 128]
            xbuf[i, rows(mr), cols] = total.astype(BF16)
        inv = lax.rsqrt(jnp.sum(square, axis=-1, keepdims=True) / dim + NORM_EPS)
        for j in range(dim // cb):
            cols = pl.ds(j * cb, cb)
            resid = slot[:, cols].astype(F32) + xbuf[i, rows(mr), cols].astype(F32)
            xbuf[i, rows(mr), cols] = (gain[:, cols] * resid * inv).astype(BF16)

    def s_copy(i, d):
        peer = (me + d) % GROUP
        return remote(sbuf.at[i, 0], sbuf.at[i, d], s_send.at[i], s_recv.at[i], (dp, peer // 4, peer % 4))

    def s_wait(i):
        block = sbuf.at[i, pl.ds(1, GROUP - 1)]
        return remote(block, block, s_send.at[i], s_recv.at[i], core_dev)

    for cp in hid_copies(0):
        cp.start()

    def load_w1(n, _):
        for cp in w1_copies(n):
            cp.start()
        return 0
    lax.fori_loop(0, ft, load_w1, 0)
    w2_copy().start()

    barrier = pltpu.get_barrier_semaphore()

    def greet(d, _):
        peer = (me + d) % GROUP
        pl.semaphore_signal(barrier, inc=1, device_id=(dp, peer // 4, peer % 4), device_id_type=MESH)
        return 0
    lax.fori_loop(1, GROUP, greet, 0)

    def gate_up(at, width):
        both = jnp.dot(hid[...], w1[:, pl.ds(at, width)], preferred_element_type=F32)
        for b in range(width // 256):
            g = both[:, b * 256:b * 256 + 128]
            up = both[:, b * 256 + 128:b * 256 + 256]
            if isinstance(at, int):
                cols = pl.ds(at // 2 + b * 128, 128)
            else:
                cols = pl.ds(pl.multiple_of(at // 2 + b * 128, 128), 128)
            act[:, cols] = (jax.nn.silu(g) * up).astype(BF16)

    def down(i, at, width):
        cols = pl.ds(at, width)
        out = jnp.dot(act[...], w2[:, cols], preferred_element_type=F32).astype(BF16)
        acc[i, :, cols] = out[:HALF]
        dsend[:, cols] = out[HALF:]

    def mlp_step(i, j):
        per = -(-ft // 4)
        if j == 0:
            for cp in hid_copies(i):
                cp.wait()
        if j < 4:
            lo, hi = j * per, min(j * per + per, ft)
            if hi > lo:
                gate_up(lo * 256, (hi - lo) * 256)
        if j == 3:
            @pl.when(i + 1 < num_chunks)
            def _():
                for cp in hid_copies(i + 1):
                    cp.start()
        if j == 4:
            d_copy(i - 1, 0).wait_send()
            d_copy(i - 1, 1).wait_send()
        if j >= 4:
            for b in range(2):
                down(i, (j - 4) * (dim // 2) + b * (dim // 4), dim // 4)
            d_copy(i, j - 4).start()

    for cp in hid_copies(0):
        cp.wait()

    def first_tile(n, _):
        for cp in w1_copies(n):
            cp.wait()
        gate_up(pl.multiple_of(n * 256, 256), 256)
        return 0
    lax.fori_loop(0, ft, first_tile, 0)
    for cp in hid_copies(1):
        cp.start()
    w2_copy().wait()
    wv_copy(0).start()
    wv_copy(1).start()
    pl.semaphore_wait(barrier, GROUP - 1)

    def first_down(part, _):
        for b in range(2):
            at = pl.multiple_of(part * (dim // 2) + b * (dim // 4), dim // 4)
            down(0, at, dim // 4)
        d_copy(0, part).start()
        return 0
    lax.fori_loop(0, 2, first_down, 0)

    def column(row_ref, i, h):
        r = row_ref[pl.ds(2 * i + (c if h == 0 else 1 - c), 1), :].astype(F32)
        return jnp.transpose(jnp.broadcast_to(r, (128, 128)))

    lanes = 128
    rb = 32

    def vocab_step(i, q):
        n = i * 4 + q
        lslot = logits.at[i % 2]
        if q == 0:
            for k in range(UNITS):
                xd_copy((i, k), KINDS[k]).wait_recv()
        wv_copy(n).wait()
        col = q * vt
        lslot[:, pl.ds(col, vt)] = jnp.dot(xbuf[i], wv[q % 2], preferred_element_type=F32)

        @pl.when(n + 2 < num_chunks * 4)
        def _():
            wv_copy(n + 2).start()

        if q == 0:
            for h in range(2):
                r = pl.ds(h * HALF, HALF)
                stat[0, r] = jnp.full((HALF, lanes), -jnp.inf, F32)
                stat[1, r] = jnp.zeros((HALF, lanes), F32)
                stat[2, r] = jnp.zeros((HALF, lanes), F32)
                stat[3, r] = jnp.zeros((HALF, lanes), F32)
                stat[4, r] = 1.0 / column(temp, i, h)
                stat[5, r] = column(ids, i, h) - (me * vocab).astype(F32)

        def block(b, _):
            r = pl.ds(pl.multiple_of(b * rb, rb), rb)
            inv_t = stat[4, r]
            want = stat[5, r] - lax.broadcasted_iota(jnp.int32, (rb, lanes), 1).astype(F32) - float(q * vt)
            old = stat[0, r]
            top = old
            parts = []
            target = stat[3, r]
            for g in range(vt // lanes):
                cols = pl.ds(col + g * lanes, lanes)
                lg = lslot[r, cols] * inv_t
                lslot[r, cols] = lg
                top = jnp.maximum(top, lg)
                target = target + jnp.where(want == float(g * lanes), lg, 0.0)
                parts.append(lg)
            scale = jnp.exp(old - top)
            total = stat[1, r] * scale
            moment = stat[2, r] * scale
            for lg in parts:
                e = jnp.exp(lg - top)
                total = total + e
                moment = moment + e * lg
            stat[0, r] = top
            stat[1, r] = total
            stat[2, r] = moment
            stat[3, r] = target
            return 0
        lax.fori_loop(0, CHUNK // rb, block, 0)

        if q == 3:
            for h in range(2):
                r = pl.ds(h * HALF, HALF)
                top = stat[0, r]
                best = jnp.max(top, axis=-1, keepdims=True)
                w = jnp.exp(top - best)
                total = jnp.sum(stat[1, r] * w, axis=-1, keepdims=True)
                moment = jnp.sum(stat[2, r] * w, axis=-1, keepdims=True)
                target = jnp.sum(stat[3, r], axis=-1, keepdims=True)
                lane = lax.broadcasted_iota(jnp.int32, (HALF, lanes), 1)
                packed = jnp.where(lane == 0, best, jnp.where(lane == 1, total, jnp.where(lane == 2, moment, target)))
                turned = jnp.transpose(packed)[:4]
                at = pl.multiple_of((c if h == 0 else 1 - c) * 4, 4)
                sbuf[i, 0, pl.ds(at, 4), :] = turned
            for d in range(1, GROUP):
                s_copy(i, d).start()

    def final_step(i):
        s_wait(i).wait_recv()
        for h in range(2):
            def pick(d, n):
                return sbuf[i, d, 4 * h + n:4 * h + n + 1, :]
            top = pick(0, 0)
            for d in range(1, GROUP):
                top = jnp.maximum(top, pick(d, 0))
            total = jnp.zeros((1, HALF), F32)
            moment = jnp.zeros((1, HALF), F32)
            target = jnp.zeros((1, HALF), F32)
            for d in range(GROUP):
                w = jnp.exp(pick(d, 0) - top)
                total = total + w * pick(d, 1)
                moment = moment + w * pick(d, 2)
                target = target + pick(d, 3)
            norm = top + jnp.log(total)
            r = pl.ds(2 * i + h, 1)
            log_norm[r, :] = norm
            entropy[r, :] = norm - moment / total
            target_logp[r, :] = target - norm

        @pl.when(i > 0)
        def _():
            for cp in out_copies(i - 1):
                cp.wait()
        for h in range(2):
            row = column(log_norm, i, h)
            stat[6, pl.ds(h * HALF, HALF)] = row

        def block(b, _):
            r = pl.ds(pl.multiple_of(b * rb, rb), rb)
            ln = stat[6, r]
            for g in range(vocab // lanes):
                cols = pl.ds(g * lanes, lanes)
                outb[r, cols] = (logits[i % 2, r, cols] - ln).astype(BF16)
            return 0
        lax.fori_loop(0, CHUNK // rb, block, 0)
        for cp in out_copies(i):
            cp.start()

    def first(kind, u):
        i, k, rs, mr, zo = geo(u, kind)
        if kind == 'A':
            if k == 0:
                d_copy(i, 0).wait_recv()
                d_copy(i, 1).wait_recv()
            add_rows(i, rs, 2 * PIECE, drecv.at[i, rows(rs, 2 * PIECE)])
            ya_copy(u).start()
        else:
            add_rows(i, rs, PIECE, drecv.at[i, rows(rs)])

            @pl.when(dist(zo) == 3)
            def _():
                z_copy(u, kind).start()

    def after_ya(u):
        i, k, rs, mr, zo = geo(u, 'A')
        ya_copy(u).wait_recv()
        add_rows(i, mr, PIECE, ybuf.at[y_index(i, k, 'A')])

        @pl.when(dist(zo) == 3)
        def _():
            z_copy(u, 'A').start()

    def relay_sum(kind, u, at):
        i, k, rs, mr, zo = geo(u, kind)

        @pl.when(dist(zo) == at)
        def _():
            z_copy(u, kind).wait_recv()
            add_rows(i, mr, PIECE, zbuf.at[flat(u)])
            z_copy(u, kind).start()
        if at == 1:
            @pl.when(dist(zo) == 0)
            def _():
                hres_copy(u, kind).start()

    def owner_sum(u):
        kind = 'B'
        i, k, rs, mr, zo = geo(u, kind)

        @pl.when(dist(zo) == 0)
        def _():
            z_copy(u, 'B').wait_recv()
            add_rows(i, mr, PIECE, zbuf.at[flat(u)])
            yb_copy(u, kind).start()

    def owner_norm(kind, u):
        i, k, rs, mr, zo = geo(u, kind)

        @pl.when(dist(zo) == 0)
        def _():
            if kind == 'A':
                z_copy(u, kind).wait_recv()
                norm_rows(u, kind, zbuf.at[flat(u)])
                x_copy(u, kind).start()
                xy_copy(u).start()
            else:
                yb_copy(u, kind).wait_recv()
                norm_rows(u, kind, ybuf.at[y_index(i, k, 'B')])
                x_copy(u, kind).start()
                xd_copy(u, kind).start()

    def relay_x(kind, u, at):
        i, k, rs, mr, zo = geo(u, kind)

        @pl.when(dist(zo) == at)
        def _():
            x_copy(u, kind).wait_recv()
            if at < 3:
                x_copy(u, kind).start()
            if kind == 'A':
                xy_copy(u).start()
            else:
                xd_copy(u, kind).start()

    def after_xy(u):
        xy_wait(u).wait_recv()
        xd_copy(u, 'A').start()

    def first_c(u):
        i, k, rs, mr, zo = geo(u, 'C')
        add_rows(i, rs, PIECE, drecv.at[i, rows(rs)])

        @pl.when(z == 3 * (2 - zo))
        def _():
            z_copy(u, 'C').start()

        @pl.when(z == 3 * (zo - 1))
        def _():
            c_copy(u).start()

    def relay_c(u):
        i, k, rs, mr, zo = geo(u, 'C')

        @pl.when(z == 3 - zo)
        def _():
            z_copy(u, 'C').wait_recv()
            add_rows(i, mr, PIECE, zbuf.at[flat(u)])
            z_copy(u, 'C').start()

        @pl.when(z == zo)
        def _():
            hres_copy(u, 'C').start()

    def owner_sum_c(u):
        kind = 'C'
        i, k, rs, mr, zo = geo(u, kind)

        @pl.when(z == zo)
        def _():
            z_copy(u, kind).wait_recv()
            c_copy(u).wait_recv()
            add_rows(i, mr, PIECE, zbuf.at[flat(u)], cbuf.at[i])
            yb_copy(u, kind).start()

    def owner_norm_c(u):
        kind = 'C'
        i, k, rs, mr, zo = geo(u, kind)

        @pl.when(z == zo)
        def _():
            yb_copy(u, kind).wait_recv()
            norm_rows(u, kind, ybuf.at[y_index(i, k, kind)])
            x_copy(u, kind).start()
            xn_copy(u).start()
            xd_copy(u, kind).start()

    def relay_x_c(u):
        i, k, rs, mr, zo = geo(u, 'C')

        @pl.when(z == 3 - zo)
        def _():
            x_copy(u, 'C').wait_recv()
            x_copy(u, 'C').start()
            xd_copy(u, 'C').start()

        @pl.when(z == 3 * (zo - 1))
        def _():
            x_copy(u, 'C').wait_recv()
            xd_copy(u, 'C').start()

    def far_x_c(u):
        i, k, rs, mr, zo = geo(u, 'C')

        @pl.when(z == 3 * (2 - zo))
        def _():
            x_copy(u, 'C').wait_recv()
            xd_copy(u, 'C').start()

    def part(f, *fixed, **named):
        return functools.partial(f, *fixed, **named)

    steps_a = (part(first, 'A'), after_ya, part(relay_sum, 'A', at=2), part(relay_sum, 'A', at=1),
               part(owner_norm, 'A'), part(relay_x, 'A', at=1), part(relay_x, 'A', at=2), part(relay_x, 'A', at=3),
               after_xy)
    steps_b = (part(first, 'B'), part(relay_sum, 'B', at=2), part(relay_sum, 'B', at=1), owner_sum,
               part(owner_norm, 'B'), part(relay_x, 'B', at=1), part(relay_x, 'B', at=2), part(relay_x, 'B', at=3))
    steps_c = (first_c, relay_c, owner_sum_c, owner_norm_c, relay_x_c, far_x_c)

    steps = {'A': steps_a, 'B': steps_b, 'C': steps_c}
    table = []
    for k in range(UNITS):
        for h, at in enumerate(POS_UNIT[k]):
            table.append((at % UNITS, at // UNITS, 0, steps[KINDS[k]][h], k))
    for j, at in enumerate(POS_MLP):
        table.append((at % UNITS, at // UNITS, 1, mlp_step, j))
    for q, at in enumerate(POS_VOCAB):
        table.append((at % UNITS, at // UNITS, 0, vocab_step, q))
    table.append((POS_FINAL % UNITS, POS_FINAL // UNITS, 0, final_step, None))
    table.sort(key=lambda row: row[:2])

    def one(i, body, n):
        if n is None:
            body(i)
        elif body in (mlp_step, vocab_step):
            body(i, n)
        else:
            body((i, n))

    def one_pass(it, _):
        for _, late, low, body, n in table:
            i = it - int(late)

            @pl.when((i >= low) & (i < num_chunks))
            def _():
                one(i, body, n)
        return 0

    passes = num_chunks + max(int(row[1]) for row in table)
    lax.fori_loop(0, passes, one_pass, 0)

    for cp in out_copies(num_chunks - 1):
        cp.wait()
    d_copy(num_chunks - 1, 0).wait_send()
    d_copy(num_chunks - 1, 1).wait_send()

    def drain_unit(u, kind):
        i, k, rs, mr, zo = geo(u, kind)
        xd_copy(u, kind).wait_send()
        if kind == 'A':
            ya_copy(u).wait_send()
            xy_copy(u).wait_send()
        own = dist(zo) == 0
        if kind == 'C':
            own = z == zo

        @pl.when(jnp.logical_not(own))
        def _():
            z_copy(u, kind).wait_send()

        @pl.when((own | (z == 3 - zo)) if kind == 'C' else dist(zo) < 3)
        def _():
            x_copy(u, kind).wait_send()

        if kind != 'A':
            @pl.when(own)
            def _():
                yb_copy(u, kind).wait_send()
                if kind == 'C':
                    xn_copy(u).wait_send()

    def drain(n, _):
        for k in range(UNITS):
            drain_unit((n, k), KINDS[k])
        return 0
    lax.fori_loop(0, num_chunks, drain, 0)

    def drain_stats(i, _):
        s_wait(i).wait_send()
        return 0
    lax.fori_loop(0, num_chunks, drain_stats, 0)


def finish(logprobs, log_norm, entropy, target_logp, out, a, b, d, block, load_sem, store_sem):
    a[...] = log_norm[...]
    b[...] = entropy[...]
    d[...] = target_logp[...]
    n, size = block.shape[0], block.shape[1]
    loads = [pltpu.make_async_copy(logprobs.at[pl.ds(j * size, size)], block.at[j], load_sem.at[j]) for j in range(n)]
    stores = [pltpu.make_async_copy(block.at[j], out.at[pl.ds(j * size, size)], store_sem.at[j]) for j in range(n)]
    for cp in loads:
        cp.start()
    for j in range(n):
        loads[j].wait()
        stores[j].start()
    for cp in stores:
        cp.wait()


def hand_over(logprobs, log_norm, entropy, target_logp):
    rows, vocab = logprobs.shape
    n = 8
    vm = pl.BlockSpec(memory_space=pltpu.VMEM)
    hbm = pl.BlockSpec(memory_space=pl.ANY)
    small = jax.ShapeDtypeStruct(log_norm.shape, F32)
    return pl.pallas_call(
        finish,
        out_shape=(jax.ShapeDtypeStruct((rows, vocab), BF16), small, small, small),
        in_specs=[hbm, vm, vm, vm],
        out_specs=(hbm, vm, vm, vm),
        scratch_shapes=[pltpu.VMEM((n, rows // n, vocab), BF16), pltpu.SemaphoreType.DMA((n,)),
                        pltpu.SemaphoreType.DMA((n,))],
        name='hand_over',
    )(logprobs, log_norm, entropy, target_logp)


def fused(hidden, w_gate, w_up, w_down, gain, w_vocab, temp, ids):
    rows, dim = hidden.shape
    ff = w_gate.shape[1]
    vocab = w_vocab.shape[1]
    nc = rows // CHUNK
    nu = nc * UNITS
    vm = pl.BlockSpec(memory_space=pltpu.VMEM)
    hbm = pl.BlockSpec(memory_space=pl.ANY)
    dma = pltpu.SemaphoreType.DMA
    small = jax.ShapeDtypeStruct((rows // 128, 128), F32)
    return pl.pallas_call(
        functools.partial(kernel, nc),
        out_shape=(jax.ShapeDtypeStruct((rows, vocab), BF16), small, small, small),
        in_specs=[hbm, hbm, hbm, hbm, vm, hbm, vm, vm],
        out_specs=(hbm, vm, vm, vm),
        scratch_shapes=[
            pltpu.VMEM((dim, 2 * ff), BF16),
            pltpu.VMEM((ff, dim), BF16),
            pltpu.VMEM((2, dim, vocab // 4), BF16),
            pltpu.VMEM((CHUNK, dim), BF16),
            pltpu.VMEM((CHUNK, ff), BF16),
            pltpu.VMEM((HALF, dim), BF16),
            pltpu.VMEM((nc, HALF, dim), BF16),
            pltpu.VMEM((nc, HALF, dim), BF16),
            pltpu.VMEM((nu, PIECE, dim), BF16),
            pltpu.VMEM((nc, PIECE, dim), BF16),
            pltpu.VMEM((nc * 4, PIECE, dim), BF16),
            pltpu.VMEM((nc, CHUNK, dim), BF16),
            pltpu.VMEM((12, PIECE, dim), BF16),
            pltpu.VMEM((2, CHUNK, vocab), F32),
            pltpu.VMEM((7, CHUNK, 128), F32),
            pltpu.VMEM((nc, GROUP, 8, HALF), F32),
            pltpu.VMEM((CHUNK, vocab), BF16),
            dma((ff // 128, 2)), dma, dma((2,)), dma((2,)), dma((12,)), dma((2,)), dma((2,)), dma((nc, 2)),
            dma((nu,)), dma((nc * 4,)), dma((nu,)), dma((nu,)), dma((nc,)), dma((nu, 2)), dma((nu,)),
            dma((nu // 3,)), dma((nu,)), dma((nu,)), dma((nc,)), dma((nc,)),
        ],
        compiler_params=pltpu.CompilerParams(collective_id=0, has_side_effects=True, vmem_limit_bytes=67043328),
        cost_estimate=pl.CostEstimate(flops=2 * rows * dim * (3 * ff + vocab),
                                      bytes_accessed=2 * dim * (3 * ff + 4 * vocab + rows),
                                      transcendentals=rows * vocab),
        name='step_tail',
    )(hidden, w_gate, w_up, w_down, gain, w_vocab, temp, ids)


def solution(mesh):
    model_axes = ('tp2', 'tp')

    def local_step(hidden, w_gate, w_up, w_down, norm_gain, w_vocab, temperature, target_ids):
        rows = hidden.shape[0]
        logprobs, log_norm, entropy, target_logp = fused(
            hidden, w_gate, w_up, w_down, norm_gain[None, :], w_vocab,
            temperature.reshape(rows // 128, 128), target_ids.reshape(rows // 128, 128))
        logprobs, log_norm, entropy, target_logp = hand_over(logprobs, log_norm, entropy, target_logp)
        return log_norm.reshape(rows), entropy.reshape(rows), target_logp.reshape(rows), logprobs

    return jax.shard_map(
        local_step, mesh=mesh,
        in_specs=(P('dp', None), P(None, model_axes), P(None, model_axes), P(model_axes, None),
                  P(None), P(None, model_axes), P('dp'), P('dp')),
        out_specs=(P('dp'), P('dp'), P('dp'), P('dp', model_axes)),
        check_vma=False)
```

```python
import functools

import jax
import jax.numpy as jnp
from jax import lax
from jax.experimental import pallas as pl
from jax.experimental.pallas import tpu as pltpu
from jax.sharding import PartitionSpec as P

NORM_EPS = 1e-6
MESH = pl.DeviceIdType.MESH
F32 = jnp.float32
BF16 = jnp.bfloat16

CHUNK = 256
HALF = 128
PIECE = 16
UNITS = 6
GROUP = 16
KINDS = 'ABBABB'
POS_UNIT = (
    (6.295, 9.934, 14.066, 22.525, 29.115, 34.033, 39.443, 42.984, 46.131),
    (6.59, 9.639, 19.18, 22.721, 26.951, 35.213, 43.672, 44.754),
    (7.377, 10.23, 14.164, 17.508, 21.148, 25.77, 33.738, 45.049),
    (7.475, 11.607, 17.902, 23.705, 29.803, 36.885, 39.541, 42.492, 47.016),
    (8.262, 12.393, 18.098, 22.623, 27.246, 33.344, 37.869, 46.426),
    (8.852, 13.574, 19.279, 23.311, 30.689, 38.557, 42.787, 46.918),
)
POS_MLP = (0.197, 1.967, 2.361, 2.656, 4.328, 4.82)
POS_VOCAB = (48, 49.082, 50.459, 53.41)
POS_FINAL = 59.7

def kernel(num_chunks, hidden, w_gate, w_up, w_down, gain, w_vocab, temp, ids,
           logprobs, log_norm, entropy, target_logp,
           w1, w2, wv, hid, act, dsend, drecv, acc, zbuf, cbuf, ybuf, xbuf, hres, logits, stat, sbuf, outb,
           w_sem, w2_sem, wv_sem, hid_sem, hres_sem, out_sem, d_send, d_recv,
           y_send, y_recv, z_send, z_recv, c_recv, x_send, x_recv, xy_recv, xd_send, xd_recv, s_send, s_recv):
    dim = hidden.shape[1]
    ff = w_gate.shape[1]
    vocab = w_vocab.shape[1]
    vt = vocab // 4
    dt = dim // 8
    num_units = num_chunks * UNITS
    ft = ff // 128

    dp = lax.axis_index('dp')
    z = lax.axis_index('tp2')
    t = lax.axis_index('tp')
    y = t // 2
    c = t % 2
    me = z * 4 + t
    core_dev = (dp, z, y * 2 + 1 - c)
    y_dev = (dp, z, (1 - y) * 2 + c)
    def dist(zo):
        return z if zo < 2 else 3 - z

    def step_dev(zo, way):
        there = z - way if zo < 2 else z + way
        return (dp, jnp.clip(there, 0, 3), t)

    def w1_copies(n):
        col = pl.multiple_of(n * 128, 128)
        at = pl.multiple_of(n * 256, 256)
        return (pltpu.make_async_copy(w_gate.at[:, pl.ds(col, 128)], w1.at[:, pl.ds(at, 128)], w_sem.at[n, 0]),
                pltpu.make_async_copy(w_up.at[:, pl.ds(col, 128)], w1.at[:, pl.ds(at + 128, 128)], w_sem.at[n, 1]))

    def w2_copy(n):
        cols = pl.ds(pl.multiple_of(n * (dim // 4), dim // 4), dim // 4)
        return pltpu.make_async_copy(w_down.at[:, cols], w2.at[:, cols], w2_sem.at[n])

    def wv_copy(n):
        q = n % 4
        b = n % 2
        return pltpu.make_async_copy(w_vocab.at[:, pl.ds(pl.multiple_of(q * vt, vt), vt)], wv.at[b], wv_sem.at[b])

    def hid_copies(i):
        own = pl.multiple_of(i * CHUNK + c * HALF, HALF)
        oth = pl.multiple_of(i * CHUNK + (1 - c) * HALF, HALF)
        return (pltpu.make_async_copy(hidden.at[pl.ds(own, HALF)], hid.at[pl.ds(0, HALF)], hid_sem.at[0]),
                pltpu.make_async_copy(hidden.at[pl.ds(oth, HALF)], hid.at[pl.ds(HALF, HALF)], hid_sem.at[1]))

    def out_copies(i):
        own = pl.multiple_of(i * CHUNK + c * HALF, HALF)
        oth = pl.multiple_of(i * CHUNK + (1 - c) * HALF, HALF)
        return (pltpu.make_async_copy(outb.at[pl.ds(0, HALF)], logprobs.at[pl.ds(own, HALF)], out_sem.at[0]),
                pltpu.make_async_copy(outb.at[pl.ds(HALF, HALF)], logprobs.at[pl.ds(oth, HALF)], out_sem.at[1]))

    def remote(src, dst, send, recv, dev):
        return pltpu.make_async_remote_copy(src_ref=src, dst_ref=dst, send_sem=send, recv_sem=recv,
                                            device_id=dev, device_id_type=MESH)

    def d_copy(i, part, pieces):
        width = dim // pieces
        start = part * width
        cols = pl.ds(start if isinstance(part, int) else pl.multiple_of(start, width), width)
        return remote(dsend.at[:, cols], drecv.at[i, :, cols], d_send.at[part], d_recv.at[i, part], core_dev)

    def d_wait(i, what):
        for pieces in (4, 2):
            @pl.when((i == 0) if pieces == 4 else (i > 0))
            def _():
                for b in range(pieces):
                    getattr(d_copy(i, b, pieces), what)()

    def geo(u, kind):
        i, k = u
        m = k % 3
        rs = 64 * (k // 3) + 16 * m + 16 * ((m + 1) // 2)
        if kind == 'A':
            return i, k, rs, rs + PIECE * y, 3 * (k // 3)
        return i, k, rs, rs, m if kind == 'C' else 3 * (m - 1)

    def flat(u):
        return u[0] * UNITS + u[1]

    def rows(start, n=PIECE):
        return pl.ds(pl.multiple_of(start, PIECE), n)

    def y_index(i, k, kind):
        return i * 4 + k // 3 + (0 if kind == 'A' else 2)

    def ya_copy(u):
        i, k, rs, mr, zo = geo(u, 'A')
        n = y_index(i, k, 'A')
        return remote(acc.at[i, rows(rs + PIECE * (1 - y))], ybuf.at[n], y_send.at[flat(u)], y_recv.at[n], y_dev)

    def yb_copy(u, kind):
        i, k, rs, mr, zo = geo(u, kind)
        n = y_index(i, k, 'B')
        return remote(acc.at[i, rows(mr)], ybuf.at[n], y_send.at[flat(u)], y_recv.at[n], y_dev)

    def z_copy(u, kind):
        i, k, rs, mr, zo = geo(u, kind)
        return remote(acc.at[i, rows(mr)], zbuf.at[flat(u)], z_send.at[flat(u)], z_recv.at[flat(u)], step_dev(zo, 1))

    def x_copy(u, kind):
        i, k, rs, mr, zo = geo(u, kind)
        block = xbuf.at[i, rows(mr)]
        return remote(block, block, x_send.at[flat(u), 0], x_recv.at[flat(u)], step_dev(zo, -1))

    def c_copy(u):
        i, k, rs, mr, zo = geo(u, 'C')
        return remote(acc.at[i, rows(mr)], cbuf.at[i], z_send.at[flat(u)], c_recv.at[i], step_dev(zo, -1))

    def xn_copy(u):
        i, k, rs, mr, zo = geo(u, 'C')
        block = xbuf.at[i, rows(mr)]
        return remote(block, block, x_send.at[flat(u), 1], x_recv.at[flat(u)], step_dev(zo, 1))

    def xy_copy(u):
        i, k, rs, mr, zo = geo(u, 'A')
        block = xbuf.at[i, rows(mr)]
        return remote(block, block, x_send.at[flat(u), 1], xy_recv.at[flat(u) // 3], y_dev)

    def xy_wait(u):
        i, k, rs, mr, zo = geo(u, 'A')
        block = xbuf.at[i, rows(rs + PIECE * (1 - y))]
        return remote(block, block, x_send.at[flat(u), 1], xy_recv.at[flat(u) // 3], y_dev)

    def xd_copy(u, kind):
        i, k, rs, mr, zo = geo(u, kind)
        n = 2 * PIECE if kind == 'A' else PIECE
        return remote(xbuf.at[i, rows(rs, n)], xbuf.at[i, rows(HALF + rs, n)], xd_send.at[flat(u)], xd_recv.at[flat(u)], core_dev)

    def hres_copy(u, kind):
        i, k, rs, mr, zo = geo(u, kind)
        row = pl.multiple_of(i * CHUNK + c * HALF + mr, PIECE)
        return pltpu.make_async_copy(hidden.at[pl.ds(row, PIECE)], hres.at[flat(u) % 12], hres_sem.at[flat(u) % 12])

    cb = min(dim, 1024)

    def add_rows(i, start, n, *terms):
        for j in range(dim // cb):
            cols = pl.ds(j * cb, cb)
            total = acc[i, rows(start, n), cols].astype(F32)
            for ref in terms:
                total = total + ref[:, cols].astype(F32)
            acc[i, rows(start, n), cols] = total.astype(BF16)

    def norm_rows(u, kind, *terms):
        i, k, rs, mr, zo = geo(u, kind)
        slot = hres.at[flat(u) % 12]
        hres_copy(u, kind).wait()
        square = jnp.zeros((PIECE, 128), F32)
        for j in range(dim // cb):
            cols = pl.ds(j * cb, cb)
            total = acc[i, rows(mr), cols].astype(F32)
            for ref in terms:
                total = total + ref[:, cols].astype(F32)
            resid = slot[:, cols].astype(F32) + total.astype(BF16).astype(F32)
            sq = resid * resid
            for b in range(cb // 128):
                square = square + sq[:, b * 128:(b + 1) * 128]
            xbuf[i, rows(mr), cols] = total.astype(BF16)
        inv = lax.rsqrt(jnp.sum(square, axis=-1, keepdims=True) / dim + NORM_EPS)
        for j in range(dim // cb):
            cols = pl.ds(j * cb, cb)
            resid = slot[:, cols].astype(F32) + xbuf[i, rows(mr), cols].astype(F32)
            xbuf[i, rows(mr), cols] = (gain[:, cols] * resid * inv).astype(BF16)

    def s_copy(i, d):
        peer = (me + d) % GROUP
        return remote(sbuf.at[i, 0], sbuf.at[i, d], s_send.at[i], s_recv.at[i], (dp, peer // 4, peer % 4))

    def s_wait(i):
        block = sbuf.at[i, pl.ds(1, GROUP - 1)]
        return remote(block, block, s_send.at[i], s_recv.at[i], core_dev)

    for cp in hid_copies(0):
        cp.start()

    def load_w1(n, _):
        for cp in w1_copies(n):
            cp.start()
        return 0
    lax.fori_loop(0, ft, load_w1, 0)

    barrier = pltpu.get_barrier_semaphore()

    def greet(d, _):
        peer = (me + d) % GROUP
        pl.semaphore_signal(barrier, inc=1, device_id=(dp, peer // 4, peer % 4), device_id_type=MESH)
        return 0
    lax.fori_loop(1, GROUP, greet, 0)

    def gate_up(at, width):
        both = jnp.dot(hid[...], w1[:, pl.ds(at, width)], preferred_element_type=F32)
        for b in range(width // 256):
            g = both[:, b * 256:b * 256 + 128]
            up = both[:, b * 256 + 128:b * 256 + 256]
            if isinstance(at, int):
                cols = pl.ds(at // 2 + b * 128, 128)
            else:
                cols = pl.ds(pl.multiple_of(at // 2 + b * 128, 128), 128)
            act[:, cols] = (jax.nn.silu(g) * up).astype(BF16)

    def down(i, at, width):
        cols = pl.ds(at, width)
        out = jnp.dot(act[...], w2[:, cols], preferred_element_type=F32).astype(BF16)
        acc[i, :, cols] = out[:HALF]
        dsend[:, cols] = out[HALF:]

    def mlp_step(i, j):
        per = -(-ft // 4)
        if j == 0:
            for cp in hid_copies(i):
                cp.wait()
        if j < 4:
            lo, hi = j * per, min(j * per + per, ft)
            if hi > lo:
                gate_up(lo * 256, (hi - lo) * 256)
        if j == 3:
            @pl.when(i + 1 < num_chunks)
            def _():
                for cp in hid_copies(i + 1):
                    cp.start()
        if j == 4:
            d_wait(i - 1, 'wait_send')
        if j >= 4:
            for b in range(2 * (j - 4), 2 * (j - 4) + 2):
                down(i, b * (dim // 4), dim // 4)
            d_copy(i, j - 4, 2).start()

    for cp in hid_copies(0):
        cp.wait()

    def first_tile(n, _):
        for cp in w1_copies(n):
            cp.wait()
        @pl.when(n >= ft - 4)
        def _():
            w2_copy(n - (ft - 4)).start()
        gate_up(pl.multiple_of(n * 256, 256), 256)
        return 0
    lax.fori_loop(0, ft, first_tile, 0)
    for cp in hid_copies(1):
        cp.start()
    pl.semaphore_wait(barrier, GROUP - 1)

    def first_down(part, _):
        w2_copy(part).wait()
        down(0, pl.multiple_of(part * (dim // 4), dim // 4), dim // 4)
        d_copy(0, part, 4).start()
        return 0
    lax.fori_loop(0, 4, first_down, 0)
    wv_copy(0).start()
    wv_copy(1).start()

    def column(row_ref, i, h):
        r = row_ref[pl.ds(2 * i + (c if h == 0 else 1 - c), 1), :].astype(F32)
        return jnp.transpose(jnp.broadcast_to(r, (128, 128)))

    lanes = 128
    rb = 32

    def vocab_step(i, q):
        n = i * 4 + q
        lslot = logits.at[i % 2]
        if q == 0:
            for k in range(UNITS):
                xd_copy((i, k), KINDS[k]).wait_recv()
        wv_copy(n).wait()
        col = q * vt
        lslot[:, pl.ds(col, vt)] = jnp.dot(xbuf[i], wv[q % 2], preferred_element_type=F32)

        @pl.when(n + 2 < num_chunks * 4)
        def _():
            wv_copy(n + 2).start()

        if q == 0:
            for h in range(2):
                r = pl.ds(h * HALF, HALF)
                stat[0, r] = jnp.full((HALF, lanes), -jnp.inf, F32)
                stat[1, r] = jnp.zeros((HALF, lanes), F32)
                stat[2, r] = jnp.zeros((HALF, lanes), F32)
                stat[3, r] = jnp.zeros((HALF, lanes), F32)
                stat[4, r] = 1.0 / column(temp, i, h)
                stat[5, r] = column(ids, i, h) - (me * vocab).astype(F32)

        def block(b, _):
            r = pl.ds(pl.multiple_of(b * rb, rb), rb)
            inv_t = stat[4, r]
            want = stat[5, r] - lax.broadcasted_iota(jnp.int32, (rb, lanes), 1).astype(F32) - float(q * vt)
            old = stat[0, r]
            top = old
            parts = []
            target = stat[3, r]
            for g in range(vt // lanes):
                cols = pl.ds(col + g * lanes, lanes)
                lg = lslot[r, cols] * inv_t
                lslot[r, cols] = lg
                top = jnp.maximum(top, lg)
                target = target + jnp.where(want == float(g * lanes), lg, 0.0)
                parts.append(lg)
            scale = jnp.exp(old - top)
            total = stat[1, r] * scale
            moment = stat[2, r] * scale
            for lg in parts:
                e = jnp.exp(lg - top)
                total = total + e
                moment = moment + e * lg
            stat[0, r] = top
            stat[1, r] = total
            stat[2, r] = moment
            stat[3, r] = target
            return 0
        lax.fori_loop(0, CHUNK // rb, block, 0)

        if q == 3:
            for h in range(2):
                r = pl.ds(h * HALF, HALF)
                top = stat[0, r]
                best = jnp.max(top, axis=-1, keepdims=True)
                w = jnp.exp(top - best)
                total = jnp.sum(stat[1, r] * w, axis=-1, keepdims=True)
                moment = jnp.sum(stat[2, r] * w, axis=-1, keepdims=True)
                target = jnp.sum(stat[3, r], axis=-1, keepdims=True)
                lane = lax.broadcasted_iota(jnp.int32, (HALF, lanes), 1)
                packed = jnp.where(lane == 0, best, jnp.where(lane == 1, total, jnp.where(lane == 2, moment, target)))
                turned = jnp.transpose(packed)[:4]
                at = pl.multiple_of((c if h == 0 else 1 - c) * 4, 4)
                sbuf[i, 0, pl.ds(at, 4), :] = turned
            for d in range(1, GROUP):
                s_copy(i, d).start()

    def final_step(i):
        s_wait(i).wait_recv()
        for h in range(2):
            def pick(d, n):
                return sbuf[i, d, 4 * h + n:4 * h + n + 1, :]
            top = pick(0, 0)
            for d in range(1, GROUP):
                top = jnp.maximum(top, pick(d, 0))
            total = jnp.zeros((1, HALF), F32)
            moment = jnp.zeros((1, HALF), F32)
            target = jnp.zeros((1, HALF), F32)
            for d in range(GROUP):
                w = jnp.exp(pick(d, 0) - top)
                total = total + w * pick(d, 1)
                moment = moment + w * pick(d, 2)
                target = target + pick(d, 3)
            norm = top + jnp.log(total)
            r = pl.ds(2 * i + h, 1)
            log_norm[r, :] = norm
            entropy[r, :] = norm - moment / total
            target_logp[r, :] = target - norm

        @pl.when(i > 0)
        def _():
            for cp in out_copies(i - 1):
                cp.wait()
        for h in range(2):
            row = column(log_norm, i, h)
            stat[6, pl.ds(h * HALF, HALF)] = row

        def block(b, _):
            r = pl.ds(pl.multiple_of(b * rb, rb), rb)
            ln = stat[6, r]
            for g in range(vocab // lanes):
                cols = pl.ds(g * lanes, lanes)
                outb[r, cols] = (logits[i % 2, r, cols] - ln).astype(BF16)
            return 0
        lax.fori_loop(0, CHUNK // rb, block, 0)
        for cp in out_copies(i):
            cp.start()

    def first(kind, u):
        i, k, rs, mr, zo = geo(u, kind)
        if kind == 'A':
            if k == 0:
                d_wait(i, 'wait_recv')
            add_rows(i, rs, 2 * PIECE, drecv.at[i, rows(rs, 2 * PIECE)])
            ya_copy(u).start()
        else:
            add_rows(i, rs, PIECE, drecv.at[i, rows(rs)])

            @pl.when(dist(zo) == 3)
            def _():
                z_copy(u, kind).start()

    def after_ya(u):
        i, k, rs, mr, zo = geo(u, 'A')
        ya_copy(u).wait_recv()
        add_rows(i, mr, PIECE, ybuf.at[y_index(i, k, 'A')])

        @pl.when(dist(zo) == 3)
        def _():
            z_copy(u, 'A').start()

    def relay_sum(kind, u, at):
        i, k, rs, mr, zo = geo(u, kind)

        @pl.when(dist(zo) == at)
        def _():
            z_copy(u, kind).wait_recv()
            add_rows(i, mr, PIECE, zbuf.at[flat(u)])
            z_copy(u, kind).start()
        if at == 1:
            @pl.when(dist(zo) == 0)
            def _():
                hres_copy(u, kind).start()

    def owner_sum(u):
        kind = 'B'
        i, k, rs, mr, zo = geo(u, kind)

        @pl.when(dist(zo) == 0)
        def _():
            z_copy(u, 'B').wait_recv()
            add_rows(i, mr, PIECE, zbuf.at[flat(u)])
            yb_copy(u, kind).start()

    def owner_norm(kind, u):
        i, k, rs, mr, zo = geo(u, kind)

        @pl.when(dist(zo) == 0)
        def _():
            if kind == 'A':
                z_copy(u, kind).wait_recv()
                norm_rows(u, kind, zbuf.at[flat(u)])
                x_copy(u, kind).start()
                xy_copy(u).start()
            else:
                yb_copy(u, kind).wait_recv()
                norm_rows(u, kind, ybuf.at[y_index(i, k, 'B')])
                x_copy(u, kind).start()
                xd_copy(u, kind).start()

    def relay_x(kind, u, at):
        i, k, rs, mr, zo = geo(u, kind)

        @pl.when(dist(zo) == at)
        def _():
            x_copy(u, kind).wait_recv()
            if at < 3:
                x_copy(u, kind).start()
            if kind == 'A':
                xy_copy(u).start()
            else:
                xd_copy(u, kind).start()

    def after_xy(u):
        xy_wait(u).wait_recv()
        xd_copy(u, 'A').start()

    def first_c(u):
        i, k, rs, mr, zo = geo(u, 'C')
        add_rows(i, rs, PIECE, drecv.at[i, rows(rs)])

        @pl.when(z == 3 * (2 - zo))
        def _():
            z_copy(u, 'C').start()

        @pl.when(z == 3 * (zo - 1))
        def _():
            c_copy(u).start()

    def relay_c(u):
        i, k, rs, mr, zo = geo(u, 'C')

        @pl.when(z == 3 - zo)
        def _():
            z_copy(u, 'C').wait_recv()
            add_rows(i, mr, PIECE, zbuf.at[flat(u)])
            z_copy(u, 'C').start()

        @pl.when(z == zo)
        def _():
            hres_copy(u, 'C').start()

    def owner_sum_c(u):
        kind = 'C'
        i, k, rs, mr, zo = geo(u, kind)

        @pl.when(z == zo)
        def _():
            z_copy(u, kind).wait_recv()
            c_copy(u).wait_recv()
            add_rows(i, mr, PIECE, zbuf.at[flat(u)], cbuf.at[i])
            yb_copy(u, kind).start()

    def owner_norm_c(u):
        kind = 'C'
        i, k, rs, mr, zo = geo(u, kind)

        @pl.when(z == zo)
        def _():
            yb_copy(u, kind).wait_recv()
            norm_rows(u, kind, ybuf.at[y_index(i, k, kind)])
            x_copy(u, kind).start()
            xn_copy(u).start()
            xd_copy(u, kind).start()

    def relay_x_c(u):
        i, k, rs, mr, zo = geo(u, 'C')

        @pl.when(z == 3 - zo)
        def _():
            x_copy(u, 'C').wait_recv()
            x_copy(u, 'C').start()
            xd_copy(u, 'C').start()

        @pl.when(z == 3 * (zo - 1))
        def _():
            x_copy(u, 'C').wait_recv()
            xd_copy(u, 'C').start()

    def far_x_c(u):
        i, k, rs, mr, zo = geo(u, 'C')

        @pl.when(z == 3 * (2 - zo))
        def _():
            x_copy(u, 'C').wait_recv()
            xd_copy(u, 'C').start()

    def part(f, *fixed, **named):
        return functools.partial(f, *fixed, **named)

    steps_a = (part(first, 'A'), after_ya, part(relay_sum, 'A', at=2), part(relay_sum, 'A', at=1),
               part(owner_norm, 'A'), part(relay_x, 'A', at=1), part(relay_x, 'A', at=2), part(relay_x, 'A', at=3),
               after_xy)
    steps_b = (part(first, 'B'), part(relay_sum, 'B', at=2), part(relay_sum, 'B', at=1), owner_sum,
               part(owner_norm, 'B'), part(relay_x, 'B', at=1), part(relay_x, 'B', at=2), part(relay_x, 'B', at=3))
    steps_c = (first_c, relay_c, owner_sum_c, owner_norm_c, relay_x_c, far_x_c)

    steps = {'A': steps_a, 'B': steps_b, 'C': steps_c}
    table = []
    for k in range(UNITS):
        for h, at in enumerate(POS_UNIT[k]):
            table.append((at % UNITS, at // UNITS, 0, steps[KINDS[k]][h], k))
    for j, at in enumerate(POS_MLP):
        table.append((at % UNITS, at // UNITS, 1, mlp_step, j))
    for q, at in enumerate(POS_VOCAB):
        table.append((at % UNITS, at // UNITS, 0, vocab_step, q))
    table.append((POS_FINAL % UNITS, POS_FINAL // UNITS, 0, final_step, None))
    table.sort(key=lambda row: row[:2])

    def one(i, body, n):
        if n is None:
            body(i)
        elif body in (mlp_step, vocab_step):
            body(i, n)
        else:
            body((i, n))

    def one_pass(it, _):
        for _, late, low, body, n in table:
            i = it - int(late)

            @pl.when((i >= low) & (i < num_chunks))
            def _():
                one(i, body, n)
        return 0

    passes = num_chunks + max(int(row[1]) for row in table)
    lax.fori_loop(0, passes, one_pass, 0)

    for cp in out_copies(num_chunks - 1):
        cp.wait()
    d_wait(num_chunks - 1, 'wait_send')

    def drain_unit(u, kind):
        i, k, rs, mr, zo = geo(u, kind)
        xd_copy(u, kind).wait_send()
        if kind == 'A':
            ya_copy(u).wait_send()
            xy_copy(u).wait_send()
        own = dist(zo) == 0
        if kind == 'C':
            own = z == zo

        @pl.when(jnp.logical_not(own))
        def _():
            z_copy(u, kind).wait_send()

        @pl.when((own | (z == 3 - zo)) if kind == 'C' else dist(zo) < 3)
        def _():
            x_copy(u, kind).wait_send()

        if kind != 'A':
            @pl.when(own)
            def _():
                yb_copy(u, kind).wait_send()
                if kind == 'C':
                    xn_copy(u).wait_send()

    def drain(n, _):
        for k in range(UNITS):
            drain_unit((n, k), KINDS[k])
        return 0
    lax.fori_loop(0, num_chunks, drain, 0)

    def drain_stats(i, _):
        s_wait(i).wait_send()
        return 0
    lax.fori_loop(0, num_chunks, drain_stats, 0)


def finish(logprobs, log_norm, entropy, target_logp, out, a, b, d, block, load_sem, store_sem):
    a[...] = log_norm[...]
    b[...] = entropy[...]
    d[...] = target_logp[...]
    n, size = block.shape[0], block.shape[1]
    loads = [pltpu.make_async_copy(logprobs.at[pl.ds(j * size, size)], block.at[j], load_sem.at[j]) for j in range(n)]
    stores = [pltpu.make_async_copy(block.at[j], out.at[pl.ds(j * size, size)], store_sem.at[j]) for j in range(n)]
    for cp in loads:
        cp.start()
    for j in range(n):
        loads[j].wait()
        stores[j].start()
    for cp in stores:
        cp.wait()


def hand_over(logprobs, log_norm, entropy, target_logp):
    rows, vocab = logprobs.shape
    n = 8
    vm = pl.BlockSpec(memory_space=pltpu.VMEM)
    hbm = pl.BlockSpec(memory_space=pl.ANY)
    small = jax.ShapeDtypeStruct(log_norm.shape, F32)
    return pl.pallas_call(
        finish,
        out_shape=(jax.ShapeDtypeStruct((rows, vocab), BF16), small, small, small),
        in_specs=[hbm, vm, vm, vm],
        out_specs=(hbm, vm, vm, vm),
        scratch_shapes=[pltpu.VMEM((n, rows // n, vocab), BF16), pltpu.SemaphoreType.DMA((n,)),
                        pltpu.SemaphoreType.DMA((n,))],
        name='hand_over',
    )(logprobs, log_norm, entropy, target_logp)


def fused(hidden, w_gate, w_up, w_down, gain, w_vocab, temp, ids):
    rows, dim = hidden.shape
    ff = w_gate.shape[1]
    vocab = w_vocab.shape[1]
    nc = rows // CHUNK
    nu = nc * UNITS
    vm = pl.BlockSpec(memory_space=pltpu.VMEM)
    hbm = pl.BlockSpec(memory_space=pl.ANY)
    dma = pltpu.SemaphoreType.DMA
    small = jax.ShapeDtypeStruct((rows // 128, 128), F32)
    return pl.pallas_call(
        functools.partial(kernel, nc),
        out_shape=(jax.ShapeDtypeStruct((rows, vocab), BF16), small, small, small),
        in_specs=[hbm, hbm, hbm, hbm, vm, hbm, vm, vm],
        out_specs=(hbm, vm, vm, vm),
        scratch_shapes=[
            pltpu.VMEM((dim, 2 * ff), BF16),
            pltpu.VMEM((ff, dim), BF16),
            pltpu.VMEM((2, dim, vocab // 4), BF16),
            pltpu.VMEM((CHUNK, dim), BF16),
            pltpu.VMEM((CHUNK, ff), BF16),
            pltpu.VMEM((HALF, dim), BF16),
            pltpu.VMEM((nc, HALF, dim), BF16),
            pltpu.VMEM((nc, HALF, dim), BF16),
            pltpu.VMEM((nu, PIECE, dim), BF16),
            pltpu.VMEM((nc, PIECE, dim), BF16),
            pltpu.VMEM((nc * 4, PIECE, dim), BF16),
            pltpu.VMEM((nc, CHUNK, dim), BF16),
            pltpu.VMEM((12, PIECE, dim), BF16),
            pltpu.VMEM((2, CHUNK, vocab), F32),
            pltpu.VMEM((7, CHUNK, 128), F32),
            pltpu.VMEM((nc, GROUP, 8, HALF), F32),
            pltpu.VMEM((CHUNK, vocab), BF16),
            dma((ff // 128, 2)), dma((4,)), dma((2,)), dma((2,)), dma((12,)), dma((2,)), dma((4,)), dma((nc, 4)),
            dma((nu,)), dma((nc * 4,)), dma((nu,)), dma((nu,)), dma((nc,)), dma((nu, 2)), dma((nu,)),
            dma((nu // 3,)), dma((nu,)), dma((nu,)), dma((nc,)), dma((nc,)),
        ],
        compiler_params=pltpu.CompilerParams(collective_id=0, has_side_effects=True, vmem_limit_bytes=67043328),
        cost_estimate=pl.CostEstimate(flops=2 * rows * dim * (3 * ff + vocab),
                                      bytes_accessed=2 * dim * (3 * ff + 4 * vocab + rows),
                                      transcendentals=rows * vocab),
        name='step_tail',
    )(hidden, w_gate, w_up, w_down, gain, w_vocab, temp, ids)


def solution(mesh):
    model_axes = ('tp2', 'tp')

    def local_step(hidden, w_gate, w_up, w_down, norm_gain, w_vocab, temperature, target_ids):
        rows = hidden.shape[0]
        logprobs, log_norm, entropy, target_logp = fused(
            hidden, w_gate, w_up, w_down, norm_gain[None, :], w_vocab,
            temperature.reshape(rows // 128, 128), target_ids.reshape(rows // 128, 128))
        logprobs, log_norm, entropy, target_logp = hand_over(logprobs, log_norm, entropy, target_logp)
        return log_norm.reshape(rows), entropy.reshape(rows), target_logp.reshape(rows), logprobs

    return jax.shard_map(
        local_step, mesh=mesh,
        in_specs=(P('dp', None), P(None, model_axes), P(None, model_axes), P(model_axes, None),
                  P(None), P(None, model_axes), P('dp'), P('dp')),
        out_specs=(P('dp'), P('dp'), P('dp'), P('dp', model_axes)),
        check_vma=False)
```
